512 devices in a mesh: groups: 2 (over y), expert: 16 (over z), split: 8 (over x), pair: 2 (over core).
Axes of the slice: x: 8, y: 2, z: 16, core: 2. Of those that a mesh axis runs over, the one named last changes fastest.
The devices are a block of a 8x8x16 slice.
Arguments:
- tokens: bfloat16 [256, 3584], P(('groups', 'expert'), ('split', 'pair')), parts along dimension 0, may hold values from -6 to 6
- routes: int32 [256, 8], P(('groups', 'expert')), parts along dimension 0, may hold values from 0 to 15, all different within a row; in each aligned block of 8 rows (0 to 7, 8 to 15, ...) at most 8 rows name the same one
- combine: float32 [256, 8], P(('groups', 'expert')), parts along dimension 0, may hold values from 0.05 to 1
- home: int32 [16], replicated, may hold values from 0 to 15, each once
- gate_up: bfloat16 [16, 3584, 2, 2560], P('expert', 'pair', None, 'split'), may hold values from -0.09375 to 0.09375
- down: bfloat16 [16, 2560, 3584], P('expert', ('split', 'pair')), may hold values from -0.15625 to 0.15625
Outputs:
- mixed: bfloat16 [256, 3584], P(('groups', 'expert'), ('split', 'pair')), parts along dimension 0
The draws below stay inside these ranges and needn't reach their ends.
There are 2 independent parts, one for each index of `groups`. The reference program is written for one: setup_inputs(seed, part) draws one part's arguments, and reference() takes and returns one part's arrays. A program takes and returns all parts, laid end to end along the dimension named above; an argument that names none is the same for every part. Nothing has to cross between parts.
Inputs may be any that keep to these rules, and one draw needn't show every extreme that they name: `routes`: each row names 8 different experts. In the rows of one device no expert is named more than 8 times, and some expert reaches 8 in every draw. A permutation: expert e is held in storage slot home[e].
All inputs are finite; a program needn't handle non-finite values.
Results may differ from the reference program's by a relative error of at most 0.025.
Values may be sent and summed in bfloat16 or wider, within the bound.
No kernel may reach another device: no remote copies, remote signals or barrier semaphores. Data moves between devices by JAX's collectives and lax.ppermute only.
A program may use at most 64 MiB of HBM per device.

```python
import math
import jax
import jax.numpy as jnp
import numpy as np
from jax import lax

D = 3584
FF = 2560
TOK_DEV = 8
EXPERTS = 16
TOPK = 8
CAP = 8
TOKENS = 128
N_SPLIT = 8
N_PAIR = 2


def spiked(drawn, own_key, source, target, shards_of, factor):
    owner, partner = [(jnp.arange(drawn.shape[dim]) // (drawn.shape[dim] // shards_of)).reshape([-1 if axis == dim else 1 for axis in range(drawn.ndim)]) for dim in (source, target)]
    chosen = jax.random.permutation(own_key, shards_of)[partner]
    strong = (owner == chosen) | (owner == (partner + shards_of // 2) % shards_of)
    return jnp.where(strong, factor * drawn, drawn)


def levels(rng, shape, split, smallest, largest):
    factor_of, own = 1.0, jax.random.fold_in(rng, 6)
    for position, parts in split:
        steps = jnp.exp(jax.random.uniform(jax.random.fold_in(own, position), (parts,), jnp.float32, smallest / len(split), largest / len(split)))
        factor_of = factor_of * jnp.repeat(steps, shape[position] // parts).reshape([-1 if axis == position else 1 for axis in range(len(shape))])
    return factor_of


def shared_out(rng, own, number, rows, count, top, bound, lean):
    sequence = jax.random.permutation(rng, count)
    heavy_load, ordinary = load_shares(count, rows * top, bound, lean, True), load_shares(count, rows * top, bound, lean, False)
    places = jnp.arange(count)

    def named(tallies, offset_by):
        used = int((tallies > 0).sum())
        fixed = max(1, used // 4)
        passed = fixed + (places - fixed + offset_by * (used - fixed)) % max(1, count - fixed)
        return jnp.zeros((count,), jnp.int32).at[sequence[jnp.where(places < fixed, places, passed)]].set(jnp.asarray(tallies, jnp.int32))

    tallies = jnp.where(number % 4 == 0, named(heavy_load, number // 4), named(ordinary, number - number // 4 - 1))
    mixed = jax.random.permutation(jax.random.fold_in(own, 3), count)
    giver, receiver = mixed[0:count // 2 * 2:2], mixed[1:count // 2 * 2:2]
    room = jnp.minimum(tallies[giver] - 1, bound - tallies[receiver]) // 2
    room = jnp.where((giver == sequence[0]) | (receiver == sequence[0]) | (tallies[receiver] == 0), 0, jnp.maximum(room, 0))
    passed = jax.random.randint(jax.random.fold_in(own, 4), (count // 2,), 0, 1 << 20) % (room + 1)
    tallies = tallies.at[giver].add(-passed).at[receiver].add(passed)
    members = jnp.searchsorted(jnp.cumsum(tallies), jnp.arange(rows * top), side="right").astype(jnp.int32)
    listing = members.reshape(top, rows).T
    listing = listing[jax.random.permutation(jax.random.fold_in(own, 1), rows)]
    offset_by = jax.random.randint(jax.random.fold_in(own, 2), (rows, 1), 0, top)
    return jnp.take_along_axis(listing, (jnp.arange(top)[None, :] + offset_by) % top, axis=1)


def load_shares(number_of, total, most, lean, full):
    portions = [(1 << 20) // math.isqrt(rank ** lean) + 1 for rank in range(1, number_of + 1)]
    largest = most if full else min(most, max(-(-total // number_of), total * portions[0] // sum(portions)))
    least = 1 if total - largest >= number_of - 1 else 0
    holding, rest = [largest] + [least] * (number_of - 1), total - largest - least * (number_of - 1)
    while rest > 0:
        movable = [i for i in range(1, number_of) if holding[i] < largest] or [i for i in range(1, number_of) if holding[i] < most]
        pool, left = sum([portions[i] for i in movable]), rest
        for i in movable:
            addition = min(most - holding[i], max(1, left * portions[i] // pool), rest)
            holding[i] = holding[i] + addition
            rest = rest - addition
    return np.array(holding)


def centred(key, shape, spread, bound, cuts=(), held_as=jnp.bfloat16):
    result = jax.random.normal(key, shape, jnp.float32) * spread
    if len(cuts) > 0:
        result = levels(key, shape, cuts, -0.22, 0.18) * result
    return jnp.clip(result, min=-bound, max=bound).astype(held_as)


def gaussian_with(own_key, shape, spread, limit, split, heavy, held_as=jnp.bfloat16):
    array = spread * jax.random.normal(own_key, shape, jnp.float32)
    if split:
        array = array * levels(own_key, shape, split, -0.22, 0.18)
    return jnp.clip(spiked(array, jax.random.fold_in(own_key, 3), *heavy), -limit, limit).astype(held_as)


def setup_inputs(seed: int = 0, part: int = 0) -> dict:
    keys = jax.random.split(jax.random.key(seed), 7)
    part_keys = jax.random.split(jax.random.fold_in(keys[6], part), 7)
    tokens = centred(part_keys[0], (TOKENS, D), 1.0, 6.0, ((0, 16), (1, 16)))
    routes_keys = jax.random.split(jax.random.fold_in(part_keys[1], 1), TOKENS // TOK_DEV)
    routes_turns = jax.random.permutation(jax.random.fold_in(part_keys[1], 3), TOKENS // TOK_DEV)
    routes = jax.vmap(lambda own, number: shared_out(jax.random.fold_in(part_keys[1], 2), own, number, TOK_DEV, EXPERTS, TOPK, CAP, 2))(routes_keys, routes_turns).reshape((TOKENS, TOPK))
    combine = jnp.clip(jnp.exp(math.log(1.0) - 2.9957323 * jax.random.uniform(part_keys[2], (TOKENS, TOPK), jnp.float32) ** levels(part_keys[2], (TOKENS, TOPK), ((0, 16),), -0.2, 0.2)), 0.05, 1.0)
    home = jax.random.permutation(keys[3], EXPERTS).astype(jnp.int32)
    gate_up = centred(keys[4], (EXPERTS, D, 2, FF), D ** -0.5, 0.09375, ((0, 16), (1, 2), (3, 8)))
    down = gaussian_with(keys[5], (EXPERTS, FF, D), FF ** -0.5, 0.15625, ((0, 16), (1, 16)), (1, 2, 16, 2.0))
    return dict(tokens=tokens, routes=routes, combine=combine, home=home, gate_up=gate_up, down=down)


def reference(tokens, routes, combine, home, gate_up, down):
    count = tokens.shape[0]
    blocks = N_SPLIT * N_PAIR
    block_width = FF // blocks
    slot = home[routes].astype(jnp.int32)

    def one_expert(index):
        weights = gate_up[index]
        gate = jnp.dot(tokens, weights[:, 0, :], preferred_element_type=jnp.float32)
        upward = jnp.dot(tokens, weights[:, 1, :], preferred_element_type=jnp.float32)
        hidden = (jax.nn.silu(gate) * upward).astype(jnp.bfloat16)
        pieces = hidden.reshape(count, blocks, block_width).astype(jnp.float32)
        down_blocks = down[index].reshape(blocks, block_width, D).astype(jnp.float32)
        partial_value = jnp.einsum('tbw,bwd->btd', pieces, down_blocks).astype(jnp.bfloat16)
        partial_value = lax.optimization_barrier(partial_value)
        return jnp.sum(partial_value.astype(jnp.float32), axis=0).astype(jnp.bfloat16)

    outputs = lax.map(one_expert, jnp.arange(EXPERTS, dtype=jnp.int32))
    chosen = (slot[:, :, None] == jnp.arange(EXPERTS, dtype=jnp.int32)[None, None, :])
    mixing = jnp.sum(jnp.where(chosen, combine[:, :, None], jnp.float32(0.0)), axis=1)
    mixed = jnp.einsum('ts,std->td', mixing, outputs.astype(jnp.float32), precision=lax.Precision.HIGHEST)
    return mixed.astype(jnp.bfloat16)
```

```python
import jax
import jax.numpy as jnp
from jax import lax
from jax.experimental import pallas as pl
from jax.experimental.pallas import tpu as pltpu
from jax.sharding import PartitionSpec as P

VMEM = pl.BlockSpec(memory_space=pltpu.VMEM)
SMEM = pl.BlockSpec(memory_space=pltpu.SMEM)
LANES = 128


def padded(value, lanes):
    rows, width = value.shape
    if width == lanes:
        return value
    return jnp.concatenate([value, jnp.zeros((rows, lanes - width), value.dtype)], axis=1)


def dispatch_kernel(home_ref, tokens_ref, routes_ref, combine_ref, out_ref):
    slots, rows, lanes = out_ref.shape
    width = tokens_ref.shape[1]
    routes = routes_ref[...]
    combine = combine_ref[...]
    slot = jnp.zeros_like(routes)
    for expert in range(slots):
        slot = jnp.where(routes == expert, home_ref[expert], slot)
    tokens = padded(tokens_ref[...].astype(jnp.float32), lanes)
    lane = lax.broadcasted_iota(jnp.int32, (rows, lanes), 1)
    for s in range(slots):
        weight = jnp.sum(jnp.where(slot == s, combine, 0.0), axis=1, keepdims=True)
        high = weight.astype(jnp.bfloat16).astype(jnp.float32)
        value = jnp.where(lane == width, high, jnp.where(lane == width + 1, weight - high, tokens))
        out_ref[s] = value.astype(jnp.bfloat16)


def arrange_kernel(pair_ref, up_ref, down_ref, up_keep, up_send, down_keep, down_send, *, width):
    even = pair_ref[0] == 0
    lanes = up_keep.shape[2]
    for ref, keep, send in ((up_ref, up_keep, up_send), (down_ref, down_keep, down_send)):
        for i in range(keep.shape[0]):
            first = padded(ref[:, 2 * i * width : (2 * i + 1) * width], lanes)
            second = padded(ref[:, (2 * i + 1) * width : (2 * i + 2) * width], lanes)
            keep[i] = jnp.where(even, first, second)
            send[i] = jnp.where(even, second, first)


def before_kernel(pair_ref, x_ref, keep_ref, recv_ref, out_ref):
    pair = pair_ref[0]
    blocks = keep_ref.shape[0]
    total = None
    for i in range(blocks):
        for ref, half in ((keep_ref, pair), (recv_ref, 1 - pair)):
            part = lax.dot_general(
                x_ref[half * blocks + i], ref[i], (((1,), (1,)), ((), ())), preferred_element_type=jnp.float32
            )
            total = part if total is None else total + part
    out_ref[...] = total.astype(out_ref.dtype)


def after_kernel(pair_ref, own_ref, other_ref, payload_ref, keep_ref, recv_ref, out_ref, *, width):
    even = pair_ref[0] == 0
    before = own_ref[...].astype(jnp.float32) + other_ref[...].astype(jnp.float32)
    units = before.shape[1] // 2
    gate, up = before[:, :units], before[:, units:]
    weight = payload_ref[:, width : width + 2].astype(jnp.float32)
    weight = weight[:, 0:1] + weight[:, 1:2]
    hidden = (gate / (1.0 + jnp.exp(-gate)) * up * weight).astype(jnp.bfloat16)
    low, high = hidden[:, : units // 2], hidden[:, units // 2 :]
    own = jnp.where(even, low, high)
    other = jnp.where(even, high, low)
    for i in range(out_ref.shape[0]):
        part = jnp.dot(own, keep_ref[i], preferred_element_type=jnp.float32)
        part = part + jnp.dot(other, recv_ref[i], preferred_element_type=jnp.float32)
        out_ref[i] = part.astype(out_ref.dtype)


def call(kernel, outs, specs, *operands):
    shapes = [jax.ShapeDtypeStruct(shape, jnp.bfloat16) for shape in outs]
    single = len(shapes) == 1
    return pl.pallas_call(
        kernel,
        out_shape=shapes[0] if single else shapes,
        in_specs=specs,
        out_specs=VMEM if single else [VMEM] * len(shapes),
    )(*operands)


def experts(tokens, routes, combine, home, gate_up, down):
    n_expert, n_split, n_pair = (lax.axis_size(name) for name in ("expert", "split", "pair"))
    rows, width = tokens.shape
    lanes = -(-(width + 2) // LANES) * LANES
    features = gate_up.shape[1]
    units = gate_up.shape[3]
    total_rows = n_expert * rows
    pair = lax.axis_index("pair").astype(jnp.int32).reshape(1)
    swap = [(0, 1), (1, 0)]

    payload = call(
        dispatch_kernel, [(n_expert, rows, lanes)], [SMEM, VMEM, VMEM, VMEM], home, tokens, routes, combine
    )
    arrived = lax.all_to_all(payload, "expert", split_axis=0, concat_axis=0, tiled=True)

    up_rows = jnp.transpose(gate_up[0], (1, 2, 0)).reshape(2 * units, features)
    down_rows = down[0]
    half_blocks = n_split // n_pair
    up_keep, up_send, down_keep, down_send = call(
        lambda *refs: arrange_kernel(*refs, width=width),
        [(half_blocks, 2 * units, lanes)] * 2 + [(n_split, down_rows.shape[0], lanes)] * 2,
        [SMEM, VMEM, VMEM],
        pair,
        up_rows,
        down_rows,
    )
    up_recv = lax.ppermute(up_send, "pair", swap)
    down_recv = lax.ppermute(down_send, "pair", swap)

    arrived = arrived.reshape(total_rows, lanes)
    spread = jnp.broadcast_to(arrived[None], (n_split, total_rows, lanes))
    gathered = lax.all_to_all(spread, "split", split_axis=0, concat_axis=0, tiled=True)
    own = call(
        before_kernel, [(total_rows, 2 * units)], [SMEM, VMEM, VMEM, VMEM], pair, gathered, up_keep, up_recv
    )
    other = lax.ppermute(own, "pair", swap)
    partial = call(
        lambda *refs: after_kernel(*refs, width=width),
        [(n_split, total_rows, lanes)],
        [SMEM] + [VMEM] * 5,
        pair,
        own,
        other,
        arrived,
        down_keep,
        down_recv,
    )
    parts = lax.all_to_all(partial, "split", split_axis=0, concat_axis=0, tiled=True)
    summed = parts.astype(jnp.float32).sum(axis=0).astype(jnp.bfloat16)
    returning = summed.reshape(n_expert, rows, lanes)
    results = lax.all_to_all(returning, "expert", split_axis=0, concat_axis=0, tiled=True)
    mixed = results.astype(jnp.float32).sum(axis=0)
    return mixed[:, :width].astype(jnp.bfloat16)


def solution(mesh):
    placed = (
        P(("groups", "expert"), ("split", "pair")),
        P(("groups", "expert"), None),
        P(("groups", "expert"), None),
        P(),
        P("expert", "pair", None, "split"),
        P("expert", ("split", "pair"), None),
    )
    return jax.shard_map(
        experts,
        mesh=mesh,
        in_specs=placed,
        out_specs=P(("groups", "expert"), ("split", "pair")),
        check_vma=False,
    )
```

```python
import jax
import jax.numpy as jnp
from jax import lax
from jax.experimental import pallas as pl
from jax.experimental.pallas import tpu as pltpu
from jax.sharding import PartitionSpec as P

VMEM = pl.BlockSpec(memory_space=pltpu.VMEM)
SMEM = pl.BlockSpec(memory_space=pltpu.SMEM)
INNER = object()
LANES = 128
GRANT = 16 << 20
BF16 = jnp.bfloat16


def padded(value, lanes):
    rows, width = value.shape
    if width == lanes:
        return value
    return jnp.concatenate([value, jnp.zeros((rows, lanes - width), value.dtype)], axis=1)


def dispatch_kernel(home_ref, tokens_ref, routes_ref, combine_ref, out_ref):
    slots, rows, lanes = out_ref.shape
    width = tokens_ref.shape[1]
    routes = routes_ref[...]
    combine = combine_ref[...]
    slot = jnp.zeros_like(routes)
    for expert in range(slots):
        slot = jnp.where(routes == expert, home_ref[expert], slot)
    tokens = padded(tokens_ref[...].astype(jnp.float32), lanes)
    lane = lax.broadcasted_iota(jnp.int32, (rows, lanes), 1)
    for s in range(slots):
        weight = jnp.sum(jnp.where(slot == s, combine, 0.0), axis=1, keepdims=True)
        high = weight.astype(jnp.bfloat16).astype(jnp.float32)
        value = jnp.where(lane == width, high, jnp.where(lane == width + 1, weight - high, tokens))
        out_ref[s] = value.astype(jnp.bfloat16)


def arrange_kernel(pair_ref, up_ref, down_ref, keep_ref, send_ref, *, width):
    even = pair_ref[0] == 0

    def cut(ref, i, turn):
        first = ref[:, 2 * i * width : (2 * i + 1) * width]
        second = ref[:, (2 * i + 1) * width : (2 * i + 2) * width]
        return (first.T, second.T) if turn else (first, second)

    row = 0
    for ref, turn in ((up_ref, False), (down_ref, True)):
        for i in range(ref.shape[1] // (2 * width)):
            first, second = cut(ref, i, turn)
            place = (pl.ds(row, first.shape[0]), pl.ds(0, first.shape[1]))
            keep_ref[place] = jnp.where(even, first, second)
            send_ref[place] = jnp.where(even, second, first)
            row += first.shape[0]


def spread_kernel(arrived_ref, x_ref, weight_ref):
    width = x_ref.shape[1]
    turned = arrived_ref[...].astype(jnp.float32).T
    tokens = turned[:width].astype(x_ref.dtype)
    for i in range(x_ref.shape[0]):
        x_ref[i] = tokens
    weight_ref[...] = turned[width : width + 1] + turned[width + 1 : width + 2]


def before_kernel(pair_ref, x_ref, keep_ref, recv_ref, out_ref):
    pair = pair_ref[0]
    blocks, width = x_ref.shape[0] // 2, x_ref.shape[1]
    rows = out_ref.shape[0]
    total = None
    for i in range(blocks):
        for ref, half in ((keep_ref, pair), (recv_ref, 1 - pair)):
            part = jnp.dot(
                ref[i * rows : (i + 1) * rows, :width],
                x_ref[half * blocks + i],
                preferred_element_type=jnp.float32,
            )
            total = part if total is None else total + part
    out_ref[...] = total.astype(out_ref.dtype)


def after_kernel(pair_ref, own_ref, other_ref, weight_ref, keep_ref, recv_ref, out_ref):
    even = pair_ref[0] == 0
    before = own_ref[...].astype(jnp.float32) + other_ref[...].astype(jnp.float32)
    units = before.shape[0] // 2
    gate, up = before[:units], before[units:]
    hidden = (gate / (1.0 + jnp.exp(-gate)) * up * weight_ref[...]).astype(jnp.bfloat16)
    depth = units // 2
    low, high = hidden[:depth], hidden[depth:]
    own = jnp.where(even, low, high)
    other = jnp.where(even, high, low)
    blocks, width, _ = out_ref.shape
    start = keep_ref.shape[0] - blocks * width
    for i in range(blocks):
        place = (pl.ds(start + i * width, width), pl.ds(0, depth))
        part = jnp.dot(keep_ref[place], own, preferred_element_type=jnp.float32)
        part = part + jnp.dot(recv_ref[place], other, preferred_element_type=jnp.float32)
        out_ref[i] = part.astype(out_ref.dtype)


def gather_kernel(parts_ref, out_ref):
    total = parts_ref[0].astype(jnp.float32)
    for i in range(1, parts_ref.shape[0]):
        total = total + parts_ref[i].astype(jnp.float32)
    out_ref[...] = total.T.astype(out_ref.dtype)


def call(kernel, outs, specs, *operands):
    outs = [pltpu.VMEM(shape, dtype) for shape, dtype in outs]
    operands = [
        pltpu.with_memory_space_constraint(operand, pltpu.VMEM) if spec is INNER else operand
        for operand, spec in zip(operands, specs)
    ]
    single = len(outs) == 1
    return pl.pallas_call(
        kernel,
        out_shape=outs[0] if single else outs,
        in_specs=[VMEM if spec is INNER else spec for spec in specs],
        out_specs=VMEM if single else [VMEM] * len(outs),
        compiler_params=pltpu.CompilerParams(vmem_limit_bytes=GRANT),
    )(*operands)


def experts(tokens, routes, combine, home, gate_up, down):
    n_expert, n_split, n_pair = (lax.axis_size(name) for name in ("expert", "split", "pair"))
    rows, width = tokens.shape
    lanes = -(-(width + 2) // LANES) * LANES
    features = gate_up.shape[1]
    units = gate_up.shape[3]
    total_rows = n_expert * rows
    pair = lax.axis_index("pair").astype(jnp.int32).reshape(1)
    swap = [(0, 1), (1, 0)]

    payload = call(
        dispatch_kernel, [((n_expert, rows, lanes), BF16)], [SMEM, VMEM, VMEM, VMEM], home, tokens, routes, combine
    )
    arrived = lax.all_to_all(payload, "expert", split_axis=0, concat_axis=0, tiled=True)

    up_rows = jnp.transpose(gate_up[0], (1, 2, 0)).reshape(2 * units, features)
    down_rows = down[0]
    arranged = (n_split // n_pair * 2 * units + n_split * width, -(-width // LANES) * LANES)
    keep, send = call(
        lambda *refs: arrange_kernel(*refs, width=width),
        [(arranged, BF16)] * 2,
        [SMEM, VMEM, VMEM],
        pair,
        up_rows,
        down_rows,
    )
    recv = lax.ppermute(send, "pair", swap)

    spread, weight = call(
        spread_kernel,
        [((n_split, width, total_rows), BF16), ((1, total_rows), jnp.float32)],
        [INNER],
        arrived.reshape(total_rows, lanes),
    )
    gathered = lax.all_to_all(spread, "split", split_axis=0, concat_axis=0, tiled=True)
    own = call(
        before_kernel,
        [((2 * units, total_rows), BF16)],
        [SMEM, INNER, INNER, INNER],
        pair,
        gathered,
        keep,
        recv,
    )
    other = lax.ppermute(own, "pair", swap)
    partial = call(
        after_kernel,
        [((n_split, width, total_rows), BF16)],
        [SMEM] + [INNER] * 5,
        pair,
        own,
        other,
        weight,
        keep,
        recv,
    )
    parts = lax.all_to_all(partial, "split", split_axis=0, concat_axis=0, tiled=True)
    returning = call(gather_kernel, [((total_rows, width), BF16)], [INNER], parts)
    results = lax.all_to_all(
        returning.reshape(n_expert, rows, width), "expert", split_axis=0, concat_axis=0, tiled=True
    )
    return results.astype(jnp.float32).sum(axis=0).astype(BF16)


def solution(mesh):
    placed = (
        P(("groups", "expert"), ("split", "pair")),
        P(("groups", "expert"), None),
        P(("groups", "expert"), None),
        P(),
        P("expert", "pair", None, "split"),
        P("expert", ("split", "pair"), None),
    )
    return jax.shard_map(
        experts,
        mesh=mesh,
        in_specs=placed,
        out_specs=P(("groups", "expert"), ("split", "pair")),
        check_vma=False,
    )
```

```python
import jax
import jax.numpy as jnp
from jax import lax
from jax.experimental import pallas as pl
from jax.experimental.pallas import tpu as pltpu
from jax.sharding import PartitionSpec as P

VMEM = pl.BlockSpec(memory_space=pltpu.VMEM)
LANES = 128
GRANT = 16 << 20
BF16 = jnp.bfloat16


def padded(value, lanes):
    rows, width = value.shape
    if width == lanes:
        return value
    return jnp.concatenate([value, jnp.zeros((rows, lanes - width), value.dtype)], axis=1)


def fetched(sources, targets, semaphores):
    copies = [
        pltpu.make_async_copy(source, target, semaphores.at[i]) for i, (source, target) in enumerate(zip(sources, targets))
    ]
    for copy in copies:
        copy.start()
    for copy in copies:
        copy.wait()


def dispatch_kernel(home_hbm, tokens_hbm, routes_hbm, combine_hbm, out_ref, home_ref, tokens_ref, routes_ref, combine_ref, semaphores):
    fetched(
        (home_hbm, tokens_hbm, routes_hbm, combine_hbm), (home_ref, tokens_ref, routes_ref, combine_ref), semaphores
    )
    slots, rows, lanes = out_ref.shape
    width = tokens_ref.shape[1]
    routes = routes_ref[...]
    combine = combine_ref[...]
    slot = jnp.zeros_like(routes)
    for expert in range(slots):
        slot = jnp.where(routes == expert, home_ref[expert], slot)
    tokens = padded(tokens_ref[...].astype(jnp.float32), lanes)
    lane = lax.broadcasted_iota(jnp.int32, (rows, lanes), 1)
    for s in range(slots):
        weight = jnp.sum(jnp.where(slot == s, combine, 0.0), axis=1, keepdims=True)
        high = weight.astype(jnp.bfloat16).astype(jnp.float32)
        value = jnp.where(lane == width, high, jnp.where(lane == width + 1, weight - high, tokens))
        out_ref[s] = value.astype(jnp.bfloat16)


def arrange_kernel(pair_ref, down_hbm, keep_ref, send_ref, down_ref, semaphores):
    fetched((down_hbm,), (down_ref,), semaphores)
    even = pair_ref[0] == 0
    width = keep_ref.shape[2]
    for i in range(keep_ref.shape[0]):
        first = down_ref[:, 2 * i * width : (2 * i + 1) * width]
        second = down_ref[:, (2 * i + 1) * width : (2 * i + 2) * width]
        keep_ref[i] = jnp.where(even, first, second)
        send_ref[i] = jnp.where(even, second, first)


def turn_kernel(arrived_ref, x_ref, weight_ref):
    width = x_ref.shape[0]
    turned = arrived_ref[...].astype(jnp.float32).T
    x_ref[...] = turned[:width].astype(x_ref.dtype)
    weight_ref[...] = turned[width : width + 1] + turned[width + 1 : width + 2]


def expert_kernel(pair_ref, x_ref, own_ref, other_ref, weight_ref, keep_ref, recv_ref, out_ref):
    pair = pair_ref[0]
    half = own_ref.shape[1]

    def part(ref, index):
        return jnp.dot(ref[...], x_ref[pl.ds(index * half, half), :], preferred_element_type=jnp.float32)

    before = part(own_ref, pair) + part(other_ref, 1 - pair)
    units = before.shape[0] // 2
    gate, up = before[:units], before[units:]
    hidden = gate / (1.0 + jnp.exp(-gate)) * up * weight_ref[...]
    even = pair == 0
    depth = units // 2
    low, high = hidden[:depth].T.astype(BF16), hidden[depth:].T.astype(BF16)
    own = jnp.where(even, low, high)
    other = jnp.where(even, high, low)
    for i in range(out_ref.shape[0]):
        total = jnp.dot(own, keep_ref[i], preferred_element_type=jnp.float32)
        total = total + jnp.dot(other, recv_ref[i], preferred_element_type=jnp.float32)
        out_ref[i] = total.T.astype(out_ref.dtype)


def gather_kernel(parts_ref, out_ref):
    total = parts_ref[0].astype(jnp.float32)
    for i in range(1, parts_ref.shape[0]):
        total = total + parts_ref[i].astype(jnp.float32)
    out_ref[...] = total.T.astype(out_ref.dtype)


def call(kernel, outs, spaces, operands, scratch=()):
    outs = [pltpu.VMEM(shape, dtype) for shape, dtype in outs]
    operands = [
        operand if space is pltpu.SMEM else pltpu.with_memory_space_constraint(operand, space)
        for operand, space in zip(operands, spaces)
    ]
    single = len(outs) == 1
    return pl.pallas_call(
        kernel,
        out_shape=outs[0] if single else outs,
        in_specs=[pl.BlockSpec(memory_space=space) for space in spaces],
        out_specs=VMEM if single else [VMEM] * len(outs),
        scratch_shapes=list(scratch),
        compiler_params=pltpu.CompilerParams(vmem_limit_bytes=GRANT),
    )(*operands)


def experts(tokens, routes, combine, home, gate_up, down):
    n_expert, n_split, _ = (lax.axis_size(name) for name in ("expert", "split", "pair"))
    rows, width = tokens.shape
    lanes = -(-(width + 2) // LANES) * LANES
    features = gate_up.shape[1]
    units = gate_up.shape[3]
    total_rows = n_expert * rows
    pair = lax.axis_index("pair").astype(jnp.int32).reshape(1)
    swap = [(0, 1), (1, 0)]
    inner, outer, scalars = pltpu.VMEM, pltpu.HBM, pltpu.SMEM

    payload = call(
        dispatch_kernel,
        [((n_expert, rows, lanes), BF16)],
        [outer] * 4,
        [home, tokens, routes, combine],
        [
            pltpu.SMEM(home.shape, home.dtype),
            pltpu.VMEM(tokens.shape, tokens.dtype),
            pltpu.VMEM(routes.shape, routes.dtype),
            pltpu.VMEM(combine.shape, combine.dtype),
            pltpu.SemaphoreType.DMA((4,)),
        ],
    )
    arrived = lax.all_to_all(payload, "expert", split_axis=0, concat_axis=0, tiled=True)

    up_own = jnp.transpose(gate_up[0], (1, 2, 0)).reshape(2 * units, features)
    up_other = lax.ppermute(up_own, "pair", swap)
    keep, send = call(
        arrange_kernel,
        [((n_split, down.shape[1], width), BF16)] * 2,
        [scalars, outer],
        [pair, down[0]],
        [pltpu.VMEM(down.shape[1:], down.dtype), pltpu.SemaphoreType.DMA((1,))],
    )
    recv = lax.ppermute(send, "pair", swap)

    turned, weight = call(
        turn_kernel,
        [((width, total_rows), BF16), ((1, total_rows), jnp.float32)],
        [inner],
        [arrived.reshape(total_rows, lanes)],
    )
    gathered = lax.all_gather(turned, ("split", "pair"), axis=0, tiled=True)
    partial = call(
        expert_kernel,
        [((n_split, width, total_rows), BF16)],
        [scalars] + [inner] * 6,
        [pair, gathered, up_own, up_other, weight, keep, recv],
    )
    parts = lax.all_to_all(partial, "split", split_axis=0, concat_axis=0, tiled=True)
    returning = call(gather_kernel, [((total_rows, width), BF16)], [inner], [parts])
    results = lax.all_to_all(
        returning.reshape(n_expert, rows, width), "expert", split_axis=0, concat_axis=0, tiled=True
    )
    return results.astype(jnp.float32).sum(axis=0).astype(BF16)


def solution(mesh):
    placed = (
        P(("groups", "expert"), ("split", "pair")),
        P(("groups", "expert"), None),
        P(("groups", "expert"), None),
        P(),
        P("expert", "pair", None, "split"),
        P("expert", ("split", "pair"), None),
    )
    return jax.shard_map(
        experts,
        mesh=mesh,
        in_specs=placed,
        out_specs=P(("groups", "expert"), ("split", "pair")),
        check_vma=False,
    )
```

```python
import jax
import jax.numpy as jnp
from jax import lax
from jax.experimental import pallas as pl
from jax.experimental.pallas import tpu as pltpu
from jax.sharding import PartitionSpec as P

VMEM = pl.BlockSpec(memory_space=pltpu.VMEM)
LANES = 128
GRANT = 16 << 20
BF16 = jnp.bfloat16


def padded(value, lanes):
    rows, width = value.shape
    if width == lanes:
        return value
    return jnp.concatenate([value, jnp.zeros((rows, lanes - width), value.dtype)], axis=1)


def fetched(sources, targets, semaphores):
    copies = [
        pltpu.make_async_copy(source, target, semaphores.at[i]) for i, (source, target) in enumerate(zip(sources, targets))
    ]
    for copy in copies:
        copy.start()
    for copy in copies:
        copy.wait()


def dispatch_kernel(home_hbm, tokens_hbm, routes_hbm, combine_hbm, out_ref, home_ref, tokens_ref, routes_ref, combine_ref, semaphores):
    fetched(
        (home_hbm, tokens_hbm, routes_hbm, combine_hbm), (home_ref, tokens_ref, routes_ref, combine_ref), semaphores
    )
    slots, rows, lanes = out_ref.shape
    width = tokens_ref.shape[1]
    routes = routes_ref[...]
    combine = combine_ref[...]
    slot = jnp.zeros_like(routes)
    for expert in range(slots):
        slot = jnp.where(routes == expert, home_ref[expert], slot)
    tokens = padded(tokens_ref[...].astype(jnp.float32), lanes)
    lane = lax.broadcasted_iota(jnp.int32, (rows, lanes), 1)
    for s in range(slots):
        weight = jnp.sum(jnp.where(slot == s, combine, 0.0), axis=1, keepdims=True)
        high = weight.astype(jnp.bfloat16).astype(jnp.float32)
        value = jnp.where(lane == width, high, jnp.where(lane == width + 1, weight - high, tokens))
        out_ref[s] = value.astype(jnp.bfloat16)


def turn_kernel(arrived_ref, x_ref, weight_ref):
    width = x_ref.shape[0]
    turned = arrived_ref[...].astype(jnp.float32).T
    x_ref[...] = turned[:width].astype(x_ref.dtype)
    weight_ref[...] = turned[width : width + 1] + turned[width + 1 : width + 2]


def expert_kernel(
    pair_ref, x_ref, up_hbm, up_other, weight_ref, down_hbm, down_other, out_ref, up_own, down_own, semaphores
):
    up_copy = pltpu.make_async_copy(up_hbm, up_own, semaphores.at[0])
    down_copy = pltpu.make_async_copy(down_hbm, down_own, semaphores.at[1])
    up_copy.start()
    down_copy.start()
    pair = pair_ref[0]
    half = up_own.shape[1]

    def part(ref, index):
        return jnp.dot(ref[...], x_ref[pl.ds(index * half, half), :], preferred_element_type=jnp.float32)

    before = part(up_other, 1 - pair)
    up_copy.wait()
    before = before + part(up_own, pair)
    units = before.shape[0] // 2
    gate, up = before[:units], before[units:]
    hidden = gate / (1.0 + jnp.exp(-gate)) * up * weight_ref[...]
    even = pair == 0
    depth = units // 2
    low, high = hidden[:depth].T.astype(BF16), hidden[depth:].T.astype(BF16)
    own = jnp.where(even, low, high)
    other = jnp.where(even, high, low)
    blocks, width, _ = out_ref.shape
    down_copy.wait()

    def blocks_of(parity):
        for i in range(blocks):
            start = (2 * i + parity) * width
            first = start // LANES * LANES
            last = -(-(start + width) // LANES) * LANES
            total = jnp.dot(own, down_own[:, first:last], preferred_element_type=jnp.float32)
            total = total + jnp.dot(other, down_other[:, first:last], preferred_element_type=jnp.float32)
            out_ref[i] = total.T[start - first : start - first + width].astype(out_ref.dtype)

    pl.when(even)(lambda: blocks_of(0))
    pl.when(jnp.logical_not(even))(lambda: blocks_of(1))


def gather_kernel(parts_ref, out_ref):
    total = parts_ref[0].astype(jnp.float32)
    for i in range(1, parts_ref.shape[0]):
        total = total + parts_ref[i].astype(jnp.float32)
    out_ref[...] = total.T.astype(out_ref.dtype)


def call(kernel, outs, spaces, operands, scratch=()):
    outs = [pltpu.VMEM(shape, dtype) for shape, dtype in outs]
    operands = [
        operand if space is pltpu.SMEM else pltpu.with_memory_space_constraint(operand, space)
        for operand, space in zip(operands, spaces)
    ]
    single = len(outs) == 1
    return pl.pallas_call(
        kernel,
        out_shape=outs[0] if single else outs,
        in_specs=[pl.BlockSpec(memory_space=space) for space in spaces],
        out_specs=VMEM if single else [VMEM] * len(outs),
        scratch_shapes=list(scratch),
        compiler_params=pltpu.CompilerParams(vmem_limit_bytes=GRANT),
    )(*operands)


def experts(tokens, routes, combine, home, gate_up, down):
    n_expert, n_split, _ = (lax.axis_size(name) for name in ("expert", "split", "pair"))
    rows, width = tokens.shape
    lanes = -(-(width + 2) // LANES) * LANES
    features = gate_up.shape[1]
    units = gate_up.shape[3]
    total_rows = n_expert * rows
    pair = lax.axis_index("pair").astype(jnp.int32).reshape(1)
    swap = [(0, 1), (1, 0)]
    inner, outer, scalars = pltpu.VMEM, pltpu.HBM, pltpu.SMEM

    payload = call(
        dispatch_kernel,
        [((n_expert, rows, lanes), BF16)],
        [outer] * 4,
        [home, tokens, routes, combine],
        [
            pltpu.SMEM(home.shape, home.dtype),
            pltpu.VMEM(tokens.shape, tokens.dtype),
            pltpu.VMEM(routes.shape, routes.dtype),
            pltpu.VMEM(combine.shape, combine.dtype),
            pltpu.SemaphoreType.DMA((4,)),
        ],
    )
    arrived = lax.all_to_all(payload, "expert", split_axis=0, concat_axis=0, tiled=True)

    up_own = jnp.transpose(gate_up[0], (1, 2, 0)).reshape(2 * units, features)
    up_other = lax.ppermute(up_own, "pair", swap)
    down_other = lax.ppermute(down[0], "pair", swap)

    turned, weight = call(
        turn_kernel,
        [((width, total_rows), BF16), ((1, total_rows), jnp.float32)],
        [inner],
        [arrived.reshape(total_rows, lanes)],
    )
    gathered = lax.all_gather(turned, ("split", "pair"), axis=0, tiled=True)
    partial = call(
        expert_kernel,
        [((n_split, width, total_rows), BF16)],
        [scalars, inner, outer, inner, inner, outer, inner],
        [pair, gathered, up_own, up_other, weight, down[0], down_other],
        [
            pltpu.VMEM(up_own.shape, up_own.dtype),
            pltpu.VMEM(down.shape[1:], down.dtype),
            pltpu.SemaphoreType.DMA((2,)),
        ],
    )
    parts = lax.all_to_all(partial, "split", split_axis=0, concat_axis=0, tiled=True)
    returning = call(gather_kernel, [((total_rows, width), BF16)], [inner], [parts])
    results = lax.all_to_all(
        returning.reshape(n_expert, rows, width), "expert", split_axis=0, concat_axis=0, tiled=True
    )
    return results.astype(jnp.float32).sum(axis=0).astype(BF16)


def solution(mesh):
    placed = (
        P(("groups", "expert"), ("split", "pair")),
        P(("groups", "expert"), None),
        P(("groups", "expert"), None),
        P(),
        P("expert", "pair", None, "split"),
        P("expert", ("split", "pair"), None),
    )
    return jax.shard_map(
        experts,
        mesh=mesh,
        in_specs=placed,
        out_specs=P(("groups", "expert"), ("split", "pair")),
        check_vma=False,
    )
```

```python
import jax
import jax.numpy as jnp
from jax import lax
from jax.experimental import pallas as pl
from jax.experimental.pallas import tpu as pltpu
from jax.sharding import PartitionSpec as P

VMEM = pl.BlockSpec(memory_space=pltpu.VMEM)
LANES = 128
GRANT = 16 << 20
BF16 = jnp.bfloat16


def padded(value, lanes):
    rows, width = value.shape
    if width == lanes:
        return value
    return jnp.concatenate([value, jnp.zeros((rows, lanes - width), value.dtype)], axis=1)


def fetched(sources, targets, semaphores):
    copies = [
        pltpu.make_async_copy(source, target, semaphores.at[i]) for i, (source, target) in enumerate(zip(sources, targets))
    ]
    for copy in copies:
        copy.start()
    for copy in copies:
        copy.wait()


def dispatch_kernel(home_hbm, tokens_hbm, routes_hbm, combine_hbm, out_ref, home_ref, tokens_ref, routes_ref, combine_ref, semaphores):
    fetched(
        (home_hbm, tokens_hbm, routes_hbm, combine_hbm), (home_ref, tokens_ref, routes_ref, combine_ref), semaphores
    )
    slots, rows, lanes = out_ref.shape
    width = tokens_ref.shape[1]
    routes = routes_ref[...]
    combine = combine_ref[...]
    slot = jnp.zeros_like(routes)
    for expert in range(slots):
        slot = jnp.where(routes == expert, home_ref[expert], slot)
    tokens = padded(tokens_ref[...].astype(jnp.float32), lanes)
    lane = lax.broadcasted_iota(jnp.int32, (rows, lanes), 1)
    for s in range(slots):
        weight = jnp.sum(jnp.where(slot == s, combine, 0.0), axis=1, keepdims=True)
        high = weight.astype(jnp.bfloat16).astype(jnp.float32)
        value = jnp.where(lane == width, high, jnp.where(lane == width + 1, weight - high, tokens))
        out_ref[s] = value.astype(jnp.bfloat16)


def turn_kernel(arrived_ref, x_ref, weight_ref):
    width = x_ref.shape[0]
    turned = arrived_ref[...].astype(jnp.float32).T
    x_ref[...] = turned[:width].astype(x_ref.dtype)
    weight_ref[...] = turned[width : width + 1] + turned[width + 1 : width + 2]


def expert_kernel(
    pair_ref,
    x_ref,
    up_hbm,
    up_other,
    weight_ref,
    down_hbm,
    down_other,
    out_ref,
    up_own,
    down_own,
    before_ref,
    up_semaphores,
    down_semaphore,
):
    rows, half = up_own.shape
    chunks = up_semaphores.shape[0]
    depth = half // chunks
    columns = [slice(i * depth, (i + 1) * depth) for i in range(chunks)]
    up_copies = [
        pltpu.make_async_copy(up_hbm.at[:, part], up_own.at[:, part], up_semaphores.at[i])
        for i, part in enumerate(columns)
    ]
    down_copy = pltpu.make_async_copy(down_hbm, down_own, down_semaphore)
    for copy in (*up_copies, down_copy):
        copy.start()
    pair = pair_ref[0]
    bands = (slice(0, rows // 2), slice(rows // 2, rows))
    x = x_ref[pl.ds((1 - pair) * half, half), :]
    for band in bands:
        before_ref[band] = jnp.dot(up_other[band], x, preferred_element_type=jnp.float32)
    for i, part in enumerate(columns):
        up_copies[i].wait()
        x = x_ref[pl.ds(pair * half + i * depth, depth), :]
        for band in bands:
            product = jnp.dot(up_own[band, part], x, preferred_element_type=jnp.float32)
            before_ref[band] = before_ref[band] + product
    before = before_ref[...]
    units = before.shape[0] // 2
    gate, up = before[:units], before[units:]
    hidden = gate / (1.0 + jnp.exp(-gate)) * up * weight_ref[...]
    even = pair == 0
    depth = units // 2
    low, high = hidden[:depth].T.astype(BF16), hidden[depth:].T.astype(BF16)
    own = jnp.where(even, low, high)
    other = jnp.where(even, high, low)
    blocks, width, _ = out_ref.shape
    down_copy.wait()

    def blocks_of(parity):
        for i in range(blocks):
            start = (2 * i + parity) * width
            first = start // LANES * LANES
            last = -(-(start + width) // LANES) * LANES
            total = jnp.dot(own, down_own[:, first:last], preferred_element_type=jnp.float32)
            total = total + jnp.dot(other, down_other[:, first:last], preferred_element_type=jnp.float32)
            out_ref[i] = total.T[start - first : start - first + width].astype(out_ref.dtype)

    pl.when(even)(lambda: blocks_of(0))
    pl.when(jnp.logical_not(even))(lambda: blocks_of(1))


def gather_kernel(parts_ref, out_ref):
    total = parts_ref[0].astype(jnp.float32)
    for i in range(1, parts_ref.shape[0]):
        total = total + parts_ref[i].astype(jnp.float32)
    out_ref[...] = total.T.astype(out_ref.dtype)


def call(kernel, outs, spaces, operands, scratch=()):
    outs = [pltpu.VMEM(shape, dtype) for shape, dtype in outs]
    operands = [
        operand if space is pltpu.SMEM else pltpu.with_memory_space_constraint(operand, space)
        for operand, space in zip(operands, spaces)
    ]
    single = len(outs) == 1
    return pl.pallas_call(
        kernel,
        out_shape=outs[0] if single else outs,
        in_specs=[pl.BlockSpec(memory_space=space) for space in spaces],
        out_specs=VMEM if single else [VMEM] * len(outs),
        scratch_shapes=list(scratch),
        compiler_params=pltpu.CompilerParams(vmem_limit_bytes=GRANT),
    )(*operands)


def experts(tokens, routes, combine, home, gate_up, down):
    n_expert, n_split, _ = (lax.axis_size(name) for name in ("expert", "split", "pair"))
    rows, width = tokens.shape
    lanes = -(-(width + 2) // LANES) * LANES
    features = gate_up.shape[1]
    units = gate_up.shape[3]
    total_rows = n_expert * rows
    pair = lax.axis_index("pair").astype(jnp.int32).reshape(1)
    swap = [(0, 1), (1, 0)]
    inner, outer, scalars = pltpu.VMEM, pltpu.HBM, pltpu.SMEM

    payload = call(
        dispatch_kernel,
        [((n_expert, rows, lanes), BF16)],
        [outer] * 4,
        [home, tokens, routes, combine],
        [
            pltpu.SMEM(home.shape, home.dtype),
            pltpu.VMEM(tokens.shape, tokens.dtype),
            pltpu.VMEM(routes.shape, routes.dtype),
            pltpu.VMEM(combine.shape, combine.dtype),
            pltpu.SemaphoreType.DMA((4,)),
        ],
    )
    arrived = lax.all_to_all(payload, "expert", split_axis=0, concat_axis=0, tiled=True)

    up_own = jnp.transpose(gate_up[0], (1, 2, 0)).reshape(2 * units, features)
    up_other = lax.ppermute(up_own, "pair", swap)
    down_other = lax.ppermute(down[0], "pair", swap)

    turned, weight = call(
        turn_kernel,
        [((width, total_rows), BF16), ((1, total_rows), jnp.float32)],
        [inner],
        [arrived.reshape(total_rows, lanes)],
    )
    gathered = lax.all_gather(turned, ("split", "pair"), axis=0, tiled=True)
    partial = call(
        expert_kernel,
        [((n_split, width, total_rows), BF16)],
        [scalars, inner, outer, inner, inner, outer, inner],
        [pair, gathered, up_own, up_other, weight, down[0], down_other],
        [
            pltpu.VMEM(up_own.shape, up_own.dtype),
            pltpu.VMEM(down.shape[1:], down.dtype),
            pltpu.VMEM((2 * units, total_rows), jnp.float32),
            pltpu.SemaphoreType.DMA((features // (2 * LANES),)),
            pltpu.SemaphoreType.DMA,
        ],
    )
    parts = lax.all_to_all(partial, "split", split_axis=0, concat_axis=0, tiled=True)
    returning = call(gather_kernel, [((total_rows, width), BF16)], [inner], [parts])
    results = lax.all_to_all(
        returning.reshape(n_expert, rows, width), "expert", split_axis=0, concat_axis=0, tiled=True
    )
    return results.astype(jnp.float32).sum(axis=0).astype(BF16)


def solution(mesh):
    placed = (
        P(("groups", "expert"), ("split", "pair")),
        P(("groups", "expert"), None),
        P(("groups", "expert"), None),
        P(),
        P("expert", "pair", None, "split"),
        P("expert", ("split", "pair"), None),
    )
    return jax.shard_map(
        experts,
        mesh=mesh,
        in_specs=placed,
        out_specs=P(("groups", "expert"), ("split", "pair")),
        check_vma=False,
    )
```
